32 devices in a mesh: wide: 8 (over z, x), narrow: 4 (over y, core).
Axes of the slice: x: 2, y: 2, z: 4, core: 2. Of those that a mesh axis runs over, the one named last changes fastest.
Arguments:
- queries: bfloat16 [4096, 2048], P(('wide', 'narrow')), may hold values from -12 to 12
- keys: bfloat16 [4096, 2048], P(('wide', 'narrow')), may hold values from -24 to 24
- values: bfloat16 [4096, 2048], P(('wide', 'narrow')), may hold values from -6 to 6
- view_lengths: int32 [8, 4], P('wide'), may hold values from 1 to 256, 512 in all within a row
- gain: float32 [2048], replicated, may hold values from 0.25 to 1.75
- w_gate: bfloat16 [4, 512, 512], P('narrow', 'wide'), may hold values from -0.25 to 0.25
- w_up: bfloat16 [4, 512, 512], P('narrow', 'wide'), may hold values from -0.25 to 0.25
- w_down: bfloat16 [4, 512, 512], P('narrow', 'wide'), may hold values from -0.25 to 0.25
- m_gate: float32 [4, 512, 512], P('narrow', 'wide'), may hold values from -4 to 4
- m_up: float32 [4, 512, 512], P('narrow', 'wide'), may hold values from -4 to 4
- m_down: float32 [4, 512, 512], P('narrow', 'wide'), may hold values from -4 to 4
Outputs:
- output: bfloat16 [4096, 2048], P(('wide', 'narrow'))
- new_gate: bfloat16 [4, 512, 512], P('narrow', 'wide')
- new_up: bfloat16 [4, 512, 512], P('narrow', 'wide')
- new_down: bfloat16 [4, 512, 512], P('narrow', 'wide')
- mom_gate: float32 [4, 512, 512], P('narrow', 'wide')
- mom_up: float32 [4, 512, 512], P('narrow', 'wide')
- mom_down: float32 [4, 512, 512], P('narrow', 'wide')
The draws below stay inside these ranges and needn't reach their ends.
Inputs may be any that keep to these rules, and one draw needn't show every extreme that they name: `view_lengths`: each row sums to 512; its largest entry is 256.
All inputs are finite; a program needn't handle non-finite values.
Results may differ from the reference program's by a relative error of at most 0.0091.
Values may be sent and summed in bfloat16 or wider, within the bound.
No kernel may reach another device: no remote copies, remote signals or barrier semaphores. Data moves between devices by JAX's collectives and lax.ppermute only.
A program may use at most 64 MiB of HBM per device.

```python
import math
import jax
import jax.numpy as jnp
import numpy as np
from jax import lax

HEAD = 512
HEADS = 4
VIEWS = 4
D = 2048
GROUP = 512
GROUPS = 8
TOKENS = 4096


def lifted_directions(key):
    base = jax.random.fold_in(key, 7001)
    flips = jax.random.bernoulli(jax.random.fold_in(base, 1), 0.5, (GROUPS, HEADS, HEAD))
    signs = jnp.where(flips, 1.0, -1.0).astype(jnp.float32)
    orders = [jax.random.permutation(jax.random.fold_in(base, 10 + number), GROUPS) for number in range(HEADS)]
    ranking = jnp.stack(orders, axis=1).astype(jnp.float32)
    chosen = max(2, GROUPS // 4)
    strength = jnp.maximum(320.0 - 210.0 * ranking / (chosen - 1), 0.0)
    amplitude = jnp.where(ranking < chosen, jnp.sqrt(strength / math.sqrt(HEAD)), 0.0)
    return signs * amplitude[:, :, None]


def noise_field(key, shape):
    return jax.random.truncated_normal(key, -6.0, 6.0, shape, jnp.float32)


def draw_queries(key, part):
    lifted = lifted_directions(key)
    noise = noise_field(jax.random.fold_in(key, 11), (GROUPS, GROUP, HEADS, HEAD))
    field = noise + lifted[:, None]
    return field.reshape(TOKENS, D).astype(jnp.bfloat16)


def draw_keys(key, part):
    lifted = lifted_directions(key)
    noise = noise_field(jax.random.fold_in(key, 12), (GROUPS, GROUP, HEADS, GROUPS, HEAD // GROUPS))
    pairing = jax.random.permutation(jax.random.fold_in(key, 13), GROUPS)
    boost = jnp.where(pairing[:, None] == jnp.arange(GROUPS)[None, :], 3.0, 1.0).astype(jnp.float32)
    field = noise * boost[:, None, None, :, None] + lifted.reshape(GROUPS, 1, HEADS, GROUPS, HEAD // GROUPS)
    return field.reshape(TOKENS, D).astype(jnp.bfloat16)


def level_of(stream_key, extent, shards, smallest, largest):
    factor_of = 1.0
    for dim, parts in shards:
        steps = jax.random.uniform(jax.random.fold_in(jax.random.fold_in(stream_key, 6), dim), (parts,), jnp.float32, smallest / len(shards), largest / len(shards))
        factor_of = factor_of * jnp.repeat(jnp.exp(steps), extent[dim] // parts).reshape((-1,) + (1,) * (len(extent) - 1 - dim))
    return factor_of


def profile(number_of, total, limit, skew):
    loads = [(1 << 20) // math.isqrt(rank ** skew) + 1 for rank in range(2, number_of + 1)]
    rest, counts = total - limit - (number_of - 1), [1] * (number_of - 1)
    while rest > 0:
        candidates = [i for i in range(number_of - 1) if counts[i] < limit]
        mass, budget = sum([loads[i] for i in candidates]), rest
        for i in candidates:
            more = min(limit - counts[i], max(1, budget * loads[i] // mass), rest)
            counts[i] = counts[i] + more
            rest = rest - more
    return np.array([limit] + counts)


def uneven_parts(stream_key, amount, total, most, slope):
    if amount == 2:
        one = jax.random.randint(stream_key, (), max(1, total - most), min(most, total - 1) + 1)
        return jnp.stack([one, total - one])
    sizes = jnp.asarray(profile(amount, total, most, slope), jnp.int32)
    couples = (amount - 1) // 2
    source_of, taker = sizes[1:1 + 2 * couples:2], sizes[2:2 + 2 * couples:2]
    margin = jnp.minimum(source_of - 1, most - taker)
    passed = jax.random.randint(jax.random.fold_in(stream_key, 1), (couples,), 0, 1 << 20) % (margin + 1)
    sizes = sizes.at[1:1 + 2 * couples:2].set(source_of - passed).at[2:2 + 2 * couples:2].set(taker + passed)
    return sizes[jax.random.permutation(jax.random.fold_in(stream_key, 2), amount)]


def normal_values(rng, shape, scale, limit, split=(), kind=jnp.bfloat16):
    entries = jax.random.normal(rng, shape, jnp.float32) * scale
    if len(split) > 0:
        entries = level_of(rng, shape, split, -0.22, 0.18) * entries
    return jnp.clip(entries, min=-limit, max=limit).astype(kind)


def setup_inputs(seed: int = 0) -> dict:
    key_of = jax.random.split(jax.random.key(seed), 12)
    return {
        "queries": draw_queries(jax.random.fold_in(key_of[11], 71), 0),
        "keys": draw_keys(jax.random.fold_in(key_of[11], 71), 0),
        "values": normal_values(key_of[2], (TOKENS, D), 1.0, 6.0, ((0, 32),)),
        "view_lengths": jax.vmap(lambda own: uneven_parts(own, VIEWS, GROUP, GROUP // 2, 1))(jax.random.split(key_of[3], GROUPS)).reshape((GROUPS, VIEWS)).astype(jnp.int32),
        "gain": jnp.clip(1.0 + 0.15 * jax.random.normal(key_of[4], (D,), jnp.float32), 0.25, 1.75),
        "w_gate": normal_values(key_of[5], (HEADS, HEAD, HEAD), HEAD ** -0.5, 0.25, ((0, 4), (1, 8))),
        "w_up": normal_values(key_of[6], (HEADS, HEAD, HEAD), HEAD ** -0.5, 0.25, ((0, 4), (1, 8))),
        "w_down": normal_values(key_of[7], (HEADS, HEAD, HEAD), HEAD ** -0.5, 0.25, ((0, 4), (1, 8))),
        "m_gate": normal_values(key_of[8], (HEADS, HEAD, HEAD), 0.5, 4.0, ((0, 4), (1, 8)), jnp.float32),
        "m_up": normal_values(key_of[9], (HEADS, HEAD, HEAD), 0.5, 4.0, ((0, 4), (1, 8)), jnp.float32),
        "m_down": normal_values(key_of[10], (HEADS, HEAD, HEAD), 0.5, 4.0, ((0, 4), (1, 8)), jnp.float32),
    }


momentum_decay = 0.9
step_size = 0.02
epsilon = 1e-06
highest_precision = lax.Precision.HIGHEST

def attend(query_rows, key_rows, value_rows, query_ids, key_ids):
    scaling = query_rows.shape[-1] ** (-0.5)
    scores = jnp.einsum('rhd,ghd->hrg', query_rows.astype(jnp.float32), key_rows.astype(jnp.float32), precision=highest_precision) * scaling
    allowed = query_ids[:, None] == key_ids[None, :]
    scores = jnp.where(allowed[None], scores, -1e+30)
    highest = lax.optimization_barrier(jnp.max(scores, axis=-1, keepdims=True))
    expo = jnp.exp(scores - highest)
    probs = (expo / lax.optimization_barrier(jnp.sum(expo, axis=-1, keepdims=True))).astype(jnp.bfloat16)
    return jnp.einsum('hrg,ghd->rhd', probs.astype(jnp.float32), value_rows.astype(jnp.float32), precision=highest_precision)

def rms_gain(field, gains):
    return field * lax.rsqrt(lax.optimization_barrier(jnp.mean(field * field, axis=-1, keepdims=True)) + epsilon) * gains

def silu_slope(pre):
    sig = jax.nn.sigmoid(pre)
    return sig * (1.0 + pre * (1.0 - sig))

def wide_dot(left, right, dims):
    return lax.dot_general(left.astype(jnp.float32), right.astype(jnp.float32), dims, precision=highest_precision, preferred_element_type=jnp.float32)

def gradients(key_rows, value_rows, gate_full, up_full, down_full):
    plain = (((1,), (0,)), ((), ()))
    pre_gate = wide_dot(key_rows, gate_full, plain)
    pre_up = wide_dot(key_rows, up_full, plain)
    activ = jax.nn.silu(pre_gate)
    hidden = (activ * pre_up).astype(jnp.bfloat16)
    d_hidden = -wide_dot(value_rows, down_full, (((1,), (1,)), ((), ())))
    d_gate = (d_hidden * pre_up * silu_slope(pre_gate)).astype(jnp.bfloat16)
    d_up = (d_hidden * activ).astype(jnp.bfloat16)
    contract = (((0,), (0,)), ((), ()))
    grad_gate = wide_dot(key_rows, d_gate, contract)
    grad_up = wide_dot(key_rows, d_up, contract)
    grad_down = -wide_dot(hidden, value_rows, contract)
    return (grad_gate, grad_up, grad_down)

def renormed(weight, moment, radius):
    old = weight.astype(jnp.float32)
    moved = old - step_size * moment / radius
    ratio = jnp.sqrt(lax.optimization_barrier(jnp.sum(old * old, axis=-1, keepdims=True)) + epsilon) / jnp.sqrt(lax.optimization_barrier(jnp.sum(moved * moved, axis=-1, keepdims=True)) + epsilon)
    return (moved * ratio).astype(jnp.bfloat16)

def apply_fast(query_rows, gate_full, up_full, down_full, gains):
    plain = (((1,), (0,)), ((), ()))
    pre_gate = wide_dot(query_rows, gate_full, plain)
    pre_up = wide_dot(query_rows, up_full, plain)
    hidden = (jax.nn.silu(pre_gate) * pre_up).astype(jnp.bfloat16)
    fast_raw = wide_dot(hidden, down_full, plain)
    return rms_gain(fast_raw, gains).astype(jnp.bfloat16)

def view_ids_of(lengths):
    ends = jnp.cumsum(lengths.astype(jnp.int32))
    position = jnp.arange(GROUP, dtype=jnp.int32)
    return lax.optimization_barrier(jnp.sum((position[:, None] >= ends[None, :-1]).astype(jnp.int32), axis=1)).astype(jnp.int32)

def reference(queries, keys, values, view_lengths, gain, w_gate, w_up, w_down, m_gate, m_up, m_down):
    head_gains = gain.reshape(HEADS, HEAD)
    grouped_q = queries.reshape(GROUPS, GROUP, HEADS, HEAD)
    grouped_k = keys.reshape(GROUPS, GROUP, HEADS, HEAD)
    grouped_v = values.reshape(GROUPS, GROUP, HEADS, HEAD)
    head_grads = jax.vmap(gradients, in_axes=(1, 1, 0, 0, 0))

    def accumulate(totals, pair):
        terms = head_grads(pair[0], pair[1], w_gate, w_up, w_down)
        return (tuple((total + term for total, term in zip(totals, terms))), None)
    zeros = jnp.zeros((HEADS, HEAD, HEAD), jnp.float32)
    grads, unused = lax.scan(accumulate, (zeros, zeros, zeros), (grouped_k, grouped_v))
    grad_scale = TOKENS ** (-0.5)
    moments = tuple((momentum_decay * moment + grad * grad_scale for moment, grad in zip((m_gate, m_up, m_down), grads)))
    fresh = tuple((renormed(weight, moment, jnp.sqrt(lax.optimization_barrier(jnp.mean(moment * moment, axis=(1, 2), keepdims=True)) + epsilon)) for weight, moment in zip((w_gate, w_up, w_down), moments)))
    head_apply = jax.vmap(apply_fast, in_axes=(1, 0, 0, 0, 0), out_axes=1)

    def group_output(inputs):
        query_rows, key_rows, value_rows, lengths = inputs
        ids = view_ids_of(lengths)
        attn = attend(query_rows, key_rows, value_rows, ids, ids)
        view_out = rms_gain(attn, head_gains).astype(jnp.bfloat16)
        fast_out = head_apply(query_rows, fresh[0], fresh[1], fresh[2], head_gains)
        return (view_out.astype(jnp.float32) + fast_out.astype(jnp.float32)).astype(jnp.bfloat16)
    output = lax.map(group_output, (grouped_q, grouped_k, grouped_v, view_lengths)).reshape(TOKENS, D)
    return (output, fresh[0], fresh[1], fresh[2], moments[0], moments[1], moments[2])
```

```python
import jax
import jax.numpy as jnp
from jax import lax
from jax.experimental import pallas as pl
from jax.experimental.pallas import tpu as pltpu
from jax.sharding import PartitionSpec as P

momentum_decay = 0.9
step_size = 0.02
epsilon = 1e-06
bf16 = jnp.bfloat16
f32 = jnp.float32


VMEM = pl.BlockSpec(memory_space=pltpu.VMEM)
SMEM = pl.BlockSpec(memory_space=pltpu.SMEM)


def shape_of(shape, dtype):
    return jax.ShapeDtypeStruct(shape, dtype)


def mm(a, b):
    return jnp.dot(a, b, preferred_element_type=f32)


def mm_nt(a, b):
    return lax.dot_general(a, b, (((1,), (1,)), ((), ())), preferred_element_type=f32)


def mm_tn(a, b):
    return lax.dot_general(a, b, (((0,), (0,)), ((), ())), preferred_element_type=f32)


class Plan:
    def __init__(self, mesh):
        self.wide = mesh.shape["wide"]
        self.narrow = mesh.shape["narrow"]
        self.direct = self.wide % 2 == 0 and self.narrow % 2 == 0 and self.wide <= 16
        self.rest = self.wide // 2

    def place(self, group, head):
        if self.direct:
            return (group // 2 * 2 + head % 2, head // 2 * 2 + group % 2)
        return (group, head)

    def role(self):
        w, n = lax.axis_index("wide"), lax.axis_index("narrow")
        if self.direct:
            return w // 2 * 2 + n % 2, n // 2 * 2 + w % 2
        return w, n

    def send(self, x, source, target):
        n = self.narrow
        pairs = []
        for a in range(self.wide):
            for b in range(self.narrow):
                s, t = source(a, b), target(a, b)
                pairs.append((s[0] * n + s[1], t[0] * n + t[1]))
        return lax.ppermute(x, ("wide", "narrow"), pairs)

    def home(self, a, b):
        return (a, b)


def assemble(dst, chunks, offsets):
    for chunk, (start, rows) in zip(chunks, offsets):
        for i in range(dst.shape[0]):
            dst[i, pl.ds(start, rows), :] = chunk[i]


def chunk_offsets(plan, rows):
    if not plan.direct:
        return [(0, rows)]
    group, _ = plan.role()
    z, c = group // 2, group % 2
    rest = plan.rest
    out = []
    for k in range(rest):
        r = lax.rem(z + rest - k, rest)
        out.append((pl.multiple_of((2 * r + c) * rows, rows), rows))
    for k in range(rest):
        r = lax.rem(z + rest - k, rest)
        out.append((pl.multiple_of((2 * r + 1 - c) * rows, rows), rows))
    return out


def grads_call(plan, kv_blocks, w_chunks):
    blocks, chunks = len(kv_blocks), len(w_chunks)
    tb, hs = kv_blocks[0].shape[1:]
    total = tb * blocks
    rows = w_chunks[0].shape[1]
    direct, rest = plan.direct, plan.rest

    def kernel(*refs):
        kv = refs[:blocks]
        ws = refs[blocks : blocks + chunks]
        w_full = refs[blocks + chunks]
        outs = refs[blocks + chunks + 1 : -5]
        k_all, v_all, hid, dg, du = refs[-5:]
        assemble(w_full, ws, chunk_offsets(plan, rows))
        for b in range(blocks):
            at = slice(b * tb, (b + 1) * tb)
            k, v = kv[b][0], kv[b][1]
            k_all[at, :] = k
            v_all[at, :] = v
            pre_gate = mm(k, w_full[0])
            pre_up = mm(k, w_full[1])
            d_hidden = -mm_nt(v, w_full[2])
            sig = 1.0 / (1.0 + jnp.exp(-pre_gate))
            activ = pre_gate * sig
            hid[at, :] = (activ * pre_up).astype(bf16)
            slope = sig * (1.0 + pre_gate * (1.0 - sig))
            dg[at, :] = (d_hidden * pre_up * slope).astype(bf16)
            du[at, :] = (d_hidden * activ).astype(bf16)
        for i, (left, right) in enumerate(((k_all, dg), (k_all, du), (hid, v_all))):
            grad = mm_tn(left[...], right[...])
            if i == 2:
                grad = -grad
            if not direct:
                outs[0][i] = grad
                continue
            part, own, tmp = outs
            tmp[i] = grad
            group, _ = plan.role()
            z, c = group // 2, group % 2
            for k in range(rest):
                r = lax.rem(z + k, rest)
                own[k, i] = tmp[i, pl.ds(pl.multiple_of((2 * r + c) * rows, rows), rows), :]
                part[k, i] = tmp[
                    i, pl.ds(pl.multiple_of((2 * r + 1 - c) * rows, rows), rows), :
                ].astype(bf16)

    out_shape = [shape_of((3, hs, hs), bf16)]
    scratch = []
    if direct:
        out_shape += [
            shape_of((rest, 3, rows, hs), bf16),
            shape_of((rest, 3, rows, hs), f32),
        ]
        scratch += [pltpu.VMEM((3, hs, hs), f32)]
    else:
        out_shape += [shape_of((3, hs, hs), f32)]
    scratch += [pltpu.VMEM((total, hs), bf16) for _ in range(5)]
    return pl.pallas_call(
        kernel,
        out_shape=out_shape,
        in_specs=[VMEM] * (blocks + chunks),
        out_specs=[VMEM] * len(out_shape),
        scratch_shapes=scratch,
        name="grads",
    )(*kv_blocks, *w_chunks)


def attend_call(plan, q_blocks, kv_blocks, lengths, gains):
    blocks = len(q_blocks)
    tb, hs = q_blocks[0].shape
    total = tb * blocks
    views = lengths.shape[1]

    def kernel(len_ref, gain_ref, *refs):
        q, kv, out = refs[:blocks], refs[blocks : 2 * blocks], refs[2 * blocks]
        k_all, v_all = refs[2 * blocks + 1 :]
        _, head = plan.role()
        gain = gain_ref[pl.ds(head, 1), :]
        ends, end = [], 0
        for i in range(views - 1):
            end = end + len_ref[0, i]
            ends.append(end)

        def view_of(pos):
            number = jnp.zeros(pos.shape, jnp.int32)
            for e in ends:
                number = number + (pos >= e).astype(jnp.int32)
            return number

        key_views = []
        for b in range(blocks):
            at = slice(b * tb, (b + 1) * tb)
            k_all[at, :] = kv[b][0]
            v_all[at, :] = kv[b][1]
            quarter = lax.rem(head + blocks - b, blocks)
            key_views.append(
                view_of(quarter * tb + lax.broadcasted_iota(jnp.int32, (1, tb), 1))
            )
        key_views = jnp.concatenate(key_views, axis=1)
        for b in range(blocks):
            quarter = lax.rem(head + blocks - b, blocks)
            row_views = view_of(quarter * tb + lax.broadcasted_iota(jnp.int32, (tb, 1), 0))
            scores = mm_nt(q[b][...], k_all[...]) * (hs ** (-0.5))
            scores = jnp.where(row_views == key_views, scores, -1e30)
            expo = jnp.exp(scores - jnp.max(scores, axis=-1, keepdims=True))
            probs = (expo / jnp.sum(expo, axis=-1, keepdims=True)).astype(bf16)
            attn = mm(probs, v_all[...])
            scale = lax.rsqrt(jnp.mean(attn * attn, axis=-1, keepdims=True) + epsilon)
            out[b] = (attn * scale * gain).astype(bf16)

    return pl.pallas_call(
        kernel,
        out_shape=shape_of((blocks, tb, hs), bf16),
        in_specs=[SMEM, VMEM] + [VMEM] * (2 * blocks),
        out_specs=VMEM,
        scratch_shapes=[pltpu.VMEM((total, hs), bf16) for _ in range(2)],
        name="attend",
    )(lengths, gains, *q_blocks, *kv_blocks)


def fast_call(plan, q_blocks, view_out, w_full, m_chunks, gains):
    blocks, chunks = len(q_blocks), len(m_chunks)
    tb, hs = q_blocks[0].shape
    rows = m_chunks[0].shape[1]
    direct = plan.direct

    def kernel(gain_ref, view_ref, w_ref, *refs):
        q = refs[:blocks]
        ms = refs[blocks : blocks + chunks]
        outs = refs[blocks + chunks : 2 * blocks + chunks]
        own = refs[2 * blocks + chunks]
        mom, new = refs[2 * blocks + chunks + 1 :]
        group, head = plan.role()
        gain = gain_ref[pl.ds(head, 1), :]
        assemble(mom, ms, chunk_offsets(plan, rows))
        part = min(128, hs)
        for i in range(3):
            squares = jnp.zeros((part, hs), f32)
            for s in range(0, hs, part):
                piece = mom[i, s : s + part, :].astype(f32)
                squares = squares + piece * piece
            radius = jnp.sqrt(jnp.sum(squares) / float(hs * hs) + epsilon)
            for s in range(0, hs, part):
                old = w_ref[i, s : s + part, :].astype(f32)
                moved = old - step_size * mom[i, s : s + part, :].astype(f32) / radius
                ratio = jnp.sqrt(
                    jnp.sum(old * old, axis=-1, keepdims=True) + epsilon
                ) / jnp.sqrt(jnp.sum(moved * moved, axis=-1, keepdims=True) + epsilon)
                new[i, s : s + part, :] = (moved * ratio).astype(bf16)
        if direct:
            start = pl.multiple_of(group * rows, rows)
            for i in range(3):
                own[i] = new[i, pl.ds(start, rows), :]
        else:
            own[...] = new[...]
        for b in range(blocks):
            pre_gate = mm(q[b][...], new[0])
            pre_up = mm(q[b][...], new[1])
            hidden = (pre_gate / (1.0 + jnp.exp(-pre_gate)) * pre_up).astype(bf16)
            raw = mm(hidden, new[2])
            scale = lax.rsqrt(jnp.mean(raw * raw, axis=-1, keepdims=True) + epsilon)
            fast = (raw * scale * gain).astype(bf16)
            outs[b][...] = (view_ref[b].astype(f32) + fast.astype(f32)).astype(bf16)

    out_shape = [shape_of((tb, hs), bf16) for _ in range(blocks)]
    out_shape += [shape_of((3, rows, hs), bf16)]
    return pl.pallas_call(
        kernel,
        out_shape=out_shape,
        in_specs=[VMEM] * (3 + blocks + chunks),
        out_specs=[VMEM] * len(out_shape),
        scratch_shapes=[pltpu.VMEM((3, hs, hs), bf16) for _ in range(2)],
        name="fast",
    )(gains, view_out, w_full, *q_blocks, *m_chunks)


def columns_call(blocks):
    count = len(blocks)
    tb, hs = blocks[0].shape

    def kernel(*refs):
        out = refs[count]
        n = lax.axis_index("narrow")
        for b in range(count):
            head = lax.rem(n + b, count)
            out[:, pl.ds(pl.multiple_of(head * hs, hs), hs)] = refs[b][...]

    return pl.pallas_call(
        kernel,
        out_shape=shape_of((tb, hs * count), bf16),
        in_specs=[VMEM] * count,
        out_specs=VMEM,
        name="columns",
    )(*blocks)


def per_device(
    plan, queries, keys, values, view_lengths, gain, w_gate, w_up, w_down, m_gate, m_up, m_down
):
    wide, narrow, rest = plan.wide, plan.narrow, plan.rest
    home, place = plan.home, plan.place
    n = lax.axis_index("narrow")
    hs = queries.shape[1] // narrow
    rows = w_gate.shape[1]
    scale = float(queries.shape[0] * narrow * wide) ** (-0.5)
    weights = jnp.stack([w_gate[0], w_up[0], w_down[0]])
    moments = jnp.stack([m_gate[0], m_up[0], m_down[0]])
    gains = gain.reshape(narrow, hs)

    def partner(x):
        return plan.send(x, place, lambda a, b: place(a ^ 1, b))

    def along(x, k):
        return plan.send(x, place, lambda a, b: place((a + 2 * k) % wide, b))

    def to_head(x, k):
        return plan.send(x, home, lambda a, b: place(a, (b + k) % narrow))

    def to_tokens(x, k):
        return plan.send(x, place, lambda a, b: (a, (b - k) % narrow))

    if plan.direct:
        w_own = [
            plan.send(weights, home, lambda a, b: place((a + 2 * k) % wide, b))
            for k in range(rest)
        ]
        w_chunks = w_own + [partner(x) for x in w_own]
    else:
        w_chunks = [lax.all_gather(weights, "wide", axis=1, tiled=True)]

    def head_columns(x, k):
        return lax.dynamic_slice_in_dim(x, (n + k) % narrow * hs, hs, x.ndim - 1)

    kv = [
        jnp.stack([head_columns(keys, k), head_columns(values, k)]) for k in range(narrow)
    ]
    kv_blocks = [to_head(x, k) for k, x in enumerate(kv)]
    queries, moments, kv_blocks = lax.optimization_barrier((queries, moments, kv_blocks))
    q_blocks = [to_head(head_columns(queries, k), k) for k in range(narrow)]
    if plan.direct:
        moments = plan.send(moments, home, place)
        lengths = plan.send(view_lengths, home, place)
    else:
        lengths = view_lengths

    grads = grads_call(plan, kv_blocks, w_chunks)
    w_full = grads[0]
    if plan.direct:
        part, own = grads[1], grads[2]
        summed = own + partner(part).astype(f32)
        got = summed[0]
        for k in range(1, rest):
            got = got + along(summed[k].astype(bf16), k).astype(f32)
        mom = momentum_decay * moments + got * scale
        m_own = [mom.astype(bf16)]
        m_own += [along(m_own[0], k) for k in range(1, rest)]
        m_chunks = m_own + [partner(x) for x in m_own]
    else:
        got = lax.psum_scatter(grads[1], "wide", scatter_dimension=1, tiled=True)
        mom = momentum_decay * moments + got * scale
        m_chunks = [lax.all_gather(mom.astype(bf16), "wide", axis=1, tiled=True)]
    view_out = attend_call(plan, q_blocks, kv_blocks, lengths, gains)
    *outs, fresh = fast_call(plan, q_blocks, view_out, w_full, m_chunks, gains)
    output = columns_call([to_tokens(x, k) for k, x in enumerate(outs)])
    if plan.direct:
        mom = plan.send(mom, place, home)
        fresh = plan.send(fresh, place, home)
    else:
        fresh = lax.dynamic_slice_in_dim(fresh, lax.axis_index("wide") * rows, rows, 1)
    return (
        output,
        fresh[0][None],
        fresh[1][None],
        fresh[2][None],
        mom[0][None],
        mom[1][None],
        mom[2][None],
    )


def solution(mesh):
    plan = Plan(mesh)

    def body(*args):
        return per_device(plan, *args)

    tokens = P(("wide", "narrow"), None)
    state = P("narrow", "wide", None)
    in_specs = (tokens, tokens, tokens, P("wide", None), P()) + (state,) * 6
    out_specs = (tokens,) + (state,) * 6
    return jax.shard_map(
        body, mesh=mesh, in_specs=in_specs, out_specs=out_specs, check_vma=False
    )
```

```python
import jax
import jax.numpy as jnp
from jax import lax
from jax.experimental import pallas as pl
from jax.experimental.pallas import tpu as pltpu
from jax.sharding import PartitionSpec as P


momentum_decay = 0.9
step_size = 0.02
epsilon = 1e-06
bf16 = jnp.bfloat16
f32 = jnp.float32


VMEM = pl.BlockSpec(memory_space=pltpu.VMEM)
SMEM = pl.BlockSpec(memory_space=pltpu.SMEM)
ANY = pl.BlockSpec(memory_space=pltpu.HBM)
PAD = 16


def shape_of(shape, dtype):
    return jax.ShapeDtypeStruct(shape, dtype)


def call(kernel, out_shape, operands, scratch=(), mib=16, smem=(), far=()):
    return pl.pallas_call(
        kernel,
        out_shape=out_shape,
        in_specs=[
            SMEM if i in smem else ANY if i in far else VMEM for i in range(len(operands))
        ],
        out_specs=[VMEM] * len(out_shape),
        scratch_shapes=list(scratch),
        compiler_params=pltpu.CompilerParams(vmem_limit_bytes=mib * 2**20),
    )(*operands)


def mm(a, b):
    return jnp.dot(a, b, preferred_element_type=f32)


def mm_nt(a, b):
    return lax.dot_general(a, b, (((1,), (1,)), ((), ())), preferred_element_type=f32)


def mm_tn(a, b):
    return lax.dot_general(a, b, (((0,), (0,)), ((), ())), preferred_element_type=f32)


class Plan:
    def __init__(self, mesh, rows, tokens, head_size, views):
        self.wide = mesh.shape["wide"]
        self.narrow = mesh.shape["narrow"]
        self.rest = self.wide // 2
        self.rows, self.tokens, self.head_size, self.views = rows, tokens, head_size, views

    def place(self, group, head):
        return (group // 2 * 2 + head % 2, head // 2 * 2 + group % 2)

    def home(self, group, head):
        return (group, head)

    def role(self):
        w, n = lax.axis_index("wide"), lax.axis_index("narrow")
        return w // 2 * 2 + n % 2, n // 2 * 2 + w % 2

    def send(self, x, source, target):
        pairs = []
        for a in range(self.wide):
            for b in range(self.narrow):
                s, t = source(a, b), target(a, b)
                pairs.append((s[0] * self.narrow + s[1], t[0] * self.narrow + t[1]))
        return lax.ppermute(x, ("wide", "narrow"), pairs)

    def partner(self, x):
        return self.send(x, self.place, lambda a, b: self.place(a ^ 1, b))

    def along(self, x, k):
        return self.send(x, self.place, lambda a, b: self.place((a + 2 * k) % self.wide, b))

    def to_head(self, x, k):
        return self.send(x, self.home, lambda a, b: self.place(a, (b + k) % self.narrow))

    def to_tokens(self, x, k):
        return self.send(x, self.place, lambda a, b: (a, (b - k) % self.narrow))

    def starts(self, k, other):
        group, _ = self.role()
        z, c = group // 2, group % 2
        r = lax.rem(z + self.rest - k, self.rest)
        return pl.multiple_of((2 * r + (1 - c if other else c)) * self.rows, self.rows)

    def goes(self, k, other):
        group, _ = self.role()
        z, c = group // 2, group % 2
        r = lax.rem(z + k, self.rest)
        return pl.multiple_of((2 * r + (1 - c if other else c)) * self.rows, self.rows)


def columns_at(plan, ref, k):
    head = lax.rem(lax.axis_index("narrow") + k, plan.narrow)
    size = plan.head_size
    return ref.at[:, pl.ds(pl.multiple_of(head * size, size), size)]


def stacked(parts):
    total, top, out = sum(x.shape[0] for x in parts), 0, None
    for x in parts:
        bottom = total - top - x.shape[0]
        padded = lax.pad(x, jnp.zeros((), x.dtype), ((top, bottom, 0), (0, 0, 0)))
        out = padded if out is None else out + padded
        top += x.shape[0]
    return out


def head_columns(plan, x, k):
    head = lax.rem(lax.axis_index("narrow") + k, plan.narrow)
    return lax.dynamic_slice_in_dim(x, head * plan.head_size, plan.head_size, 1)


def pack_queries(plan, lengths, queries, moments):
    rows, tb, hs = plan.rows, plan.tokens, plan.head_size

    def kernel(len_ref, q_ref, *refs):
        ms, first, others = refs[:3], refs[3], refs[4:]
        first[:tb, :] = columns_at(plan, q_ref, 0)[...]
        for i in range(3):
            first[tb + i * rows : tb + (i + 1) * rows, :] = ms[i][0].astype(bf16)
        line = lax.broadcasted_iota(jnp.int32, (PAD, hs), 0)
        table = jnp.zeros((PAD, hs), jnp.int32)
        for i in range(plan.views):
            table = jnp.where(line == i, len_ref[0, i], table)
        first[tb + 3 * rows :, :] = table.astype(f32).astype(bf16)
        for k, out in enumerate(others):
            out[...] = columns_at(plan, q_ref, k + 1)[...]

    shapes = [shape_of((tb + 3 * rows + PAD, hs), bf16)]
    shapes += [shape_of((tb, hs), bf16)] * (plan.narrow - 1)
    return call(kernel, shapes, [lengths, queries, *moments], mib=8, smem=(0,))


def grads_call(plan, kv, w_own, w_other):
    rows, tb, hs = plan.rows, plan.tokens, plan.head_size
    blocks, rest = plan.narrow, plan.rest
    total = blocks * tb

    def kernel(*refs):
        kv = refs[:blocks]
        w_own = refs[blocks : blocks + rest - 1]
        w_other = refs[blocks + rest - 1 : blocks + 2 * rest - 1]
        w_full, part, own, tmp, k_all, v_all, hid, dg, du = refs[blocks + 2 * rest - 1 :]
        for other, chunks in enumerate(((kv[0], *w_own), w_other)):
            for k, chunk in enumerate(chunks):
                at = plan.starts(k, other)
                for i in range(3):
                    if k == 0:
                        first = 2 * tb + i * rows
                        piece = chunk[first : first + rows, :]
                    else:
                        piece = chunk[i]
                    w_full[i, pl.ds(at, rows), :] = piece
        for b in range(blocks):
            at = slice(b * tb, (b + 1) * tb)
            k, v = kv[b][:tb, :], kv[b][tb : 2 * tb, :]
            k_all[at, :] = k
            v_all[at, :] = v
            pre_gate = mm(k, w_full[0])
            pre_up = mm(k, w_full[1])
            d_hidden = -mm_nt(v, w_full[2])
            sig = 1.0 / (1.0 + jnp.exp(-pre_gate))
            activ = pre_gate * sig
            hid[at, :] = (activ * pre_up).astype(bf16)
            slope = sig * (1.0 + pre_gate * (1.0 - sig))
            dg[at, :] = (d_hidden * pre_up * slope).astype(bf16)
            du[at, :] = (d_hidden * activ).astype(bf16)
        for i, (left, right) in enumerate(((k_all, dg), (k_all, du), (hid, v_all))):
            grad = mm_tn(left[...], right[...])
            tmp[i] = -grad if i == 2 else grad
            for k in range(rest):
                own[k, i] = tmp[i, pl.ds(plan.goes(k, 0), rows), :]
                part[k, i] = tmp[i, pl.ds(plan.goes(k, 1), rows), :].astype(bf16)

    shapes = [
        shape_of((3, hs, hs), bf16),
        shape_of((rest, 3, rows, hs), bf16),
        shape_of((rest, 3, rows, hs), f32),
    ]
    scratch = [pltpu.VMEM((3, hs, hs), f32)]
    scratch += [pltpu.VMEM((total, hs), bf16) for _ in range(5)]
    return call(kernel, shapes, [*kv, *w_own, *w_other], scratch, mib=20)


def share_call(plan, own, part):
    rows, hs, rest = plan.rows, plan.head_size, plan.rest

    def kernel(own_ref, part_ref, kept, *outs):
        kept[...] = own_ref[0] + part_ref[0].astype(f32)
        for k, out in enumerate(outs):
            out[...] = (own_ref[k + 1] + part_ref[k + 1].astype(f32)).astype(bf16)

    shapes = [shape_of((3, rows, hs), f32)] + [shape_of((3, rows, hs), bf16)] * (rest - 1)
    return call(kernel, shapes, [own, part], mib=4)


def moment_call(plan, kept, arrived, first_q, scale):
    rows, tb, hs = plan.rows, plan.tokens, plan.head_size

    def kernel(kept_ref, q_ref, *refs):
        arrived, got, mom = refs[:-2], refs[-2], refs[-1]
        for i in range(3):
            grad = kept_ref[i]
            for x in arrived:
                grad = grad + x[i].astype(f32)
            grad = grad * scale
            got[i] = grad
            old = q_ref[tb + i * rows : tb + (i + 1) * rows, :].astype(f32)
            mom[i] = (momentum_decay * old + grad).astype(bf16)

    shapes = [shape_of((3, rows, hs), f32), shape_of((3, rows, hs), bf16)]
    return call(kernel, shapes, [kept, first_q, *arrived], mib=4)


def attend_call(plan, q, kv, gains):
    rows, tb, hs = plan.rows, plan.tokens, plan.head_size
    blocks = plan.narrow

    def kernel(gain_ref, *refs):
        q, kv, out = refs[:blocks], refs[blocks : 2 * blocks], refs[2 * blocks]
        k_all, v_all = refs[2 * blocks + 1 :]
        _, head = plan.role()
        gain = gain_ref[:, pl.ds(pl.multiple_of(head * hs, hs), hs)]
        table = q[0][tb + 3 * rows :, :].astype(f32)
        ends, end = [], 0.0
        for i in range(plan.views - 1):
            end = end + table[i : i + 1, :1]
            ends.append(end)

        def view_of(pos):
            number = jnp.zeros(pos.shape, f32)
            for e in ends:
                number = number + (pos.astype(f32) >= e).astype(f32)
            return number

        key_views = []
        for b in range(blocks):
            at = slice(b * tb, (b + 1) * tb)
            k_all[at, :] = kv[b][:tb, :]
            v_all[at, :] = kv[b][tb : 2 * tb, :]
            quarter = lax.rem(head + blocks - b, blocks)
            key_views.append(
                view_of(quarter * tb + lax.broadcasted_iota(jnp.int32, (1, tb), 1))
            )
        key_views = jnp.concatenate(key_views, axis=1)
        for b in range(blocks):
            quarter = lax.rem(head + blocks - b, blocks)
            row_views = view_of(quarter * tb + lax.broadcasted_iota(jnp.int32, (tb, 1), 0))
            scores = mm_nt(q[b][:tb, :], k_all[...]) * (hs ** (-0.5))
            scores = jnp.where(row_views == key_views, scores, -1e30)
            expo = jnp.exp(scores - jnp.max(scores, axis=-1, keepdims=True))
            probs = (expo / jnp.sum(expo, axis=-1, keepdims=True)).astype(bf16)
            attn = mm(probs, v_all[...])
            norm = lax.rsqrt(jnp.mean(attn * attn, axis=-1, keepdims=True) + epsilon)
            out[b] = (attn * norm * gain).astype(bf16)

    shapes = [shape_of((blocks, tb, hs), bf16)]
    scratch = [pltpu.VMEM((blocks * tb, hs), bf16) for _ in range(2)]
    return call(kernel, shapes, [gains, *q, *kv], scratch, mib=14)[0]


def fast_call(plan, q, view_out, w_full, m_own, m_other, gains):
    rows, tb, hs = plan.rows, plan.tokens, plan.head_size
    blocks, rest = plan.narrow, plan.rest

    def kernel(gain_ref, view_ref, w_ref, *refs):
        q = refs[:blocks]
        chunks = refs[blocks : blocks + 2 * rest]
        outs = refs[blocks + 2 * rest : 2 * blocks + 2 * rest]
        mom, new = refs[2 * blocks + 2 * rest :]
        group, head = plan.role()
        gain = gain_ref[:, pl.ds(pl.multiple_of(head * hs, hs), hs)]
        for j, chunk in enumerate(chunks):
            at = plan.starts(j % rest, j // rest)
            for i in range(3):
                mom[i, pl.ds(at, rows), :] = chunk[i]
        part = min(128, hs)
        for i in range(3):
            squares = jnp.zeros((part, hs), f32)
            for s in range(0, hs, part):
                piece = mom[i, s : s + part, :].astype(f32)
                squares = squares + piece * piece
            radius = jnp.sqrt(jnp.sum(squares) / float(hs * hs) + epsilon)
            for s in range(0, hs, part):
                old = w_ref[i, s : s + part, :].astype(f32)
                moved = old - step_size * mom[i, s : s + part, :].astype(f32) / radius
                ratio = jnp.sqrt(
                    jnp.sum(old * old, axis=-1, keepdims=True) + epsilon
                ) / jnp.sqrt(jnp.sum(moved * moved, axis=-1, keepdims=True) + epsilon)
                new[i, s : s + part, :] = (moved * ratio).astype(bf16)
        start = pl.multiple_of(group * rows, rows)
        for i in range(3):
            outs[0][tb + i * rows : tb + (i + 1) * rows, :] = new[i, pl.ds(start, rows), :]
        for b in range(blocks):
            rows_q = q[b][:tb, :]
            pre_gate = mm(rows_q, new[0])
            pre_up = mm(rows_q, new[1])
            hidden = (pre_gate / (1.0 + jnp.exp(-pre_gate)) * pre_up).astype(bf16)
            raw = mm(hidden, new[2])
            norm = lax.rsqrt(jnp.mean(raw * raw, axis=-1, keepdims=True) + epsilon)
            fast = (raw * norm * gain).astype(bf16)
            outs[b][:tb, :] = (view_ref[b].astype(f32) + fast.astype(f32)).astype(bf16)

    shapes = [shape_of((tb + 3 * rows, hs), bf16)]
    shapes += [shape_of((tb, hs), bf16)] * (blocks - 1)
    scratch = [pltpu.VMEM((3, hs, hs), bf16) for _ in range(2)]
    operands = [gains, view_out, w_full, *q, *m_own, *m_other]
    return call(kernel, shapes, operands, scratch, mib=18)


def finish_call(plan, blocks):
    rows, tb, hs = plan.rows, plan.tokens, plan.head_size
    count = plan.narrow

    def kernel(*refs):
        out, fresh = refs[count], refs[count + 1 :]
        n = lax.axis_index("narrow")
        for b in range(count):
            head = lax.rem(n + b, count)
            out[:, pl.ds(pl.multiple_of(head * hs, hs), hs)] = refs[b][:tb, :]
        for i in range(3):
            fresh[i][0] = refs[0][tb + i * rows : tb + (i + 1) * rows, :]

    shapes = [shape_of((tb, hs * count), bf16)] + [shape_of((1, rows, hs), bf16)] * 3
    return call(kernel, shapes, blocks, mib=6)


def per_device(
    plan, queries, keys, values, view_lengths, gain, w_gate, w_up, w_down, m_gate, m_up, m_down
):
    narrow, rest = plan.narrow, plan.rest
    scale = float(plan.tokens * narrow * plan.wide) ** (-0.5)
    gains = gain.reshape(1, narrow * plan.head_size)
    moments = (m_gate, m_up, m_down)

    weights = [w_gate, w_up, w_down]
    flat_w = [x[0] for x in weights]
    packed_w = stacked(flat_w).reshape(3, plan.rows, plan.head_size)
    w_own = [
        plan.send(packed_w, plan.home, lambda a, b: plan.place((a + 2 * k) % plan.wide, b))
        for k in range(1, rest)
    ]
    pairs = []
    for k in range(narrow):
        parts = [head_columns(plan, keys, k), head_columns(plan, values, k)]
        pairs.append(stacked(parts + flat_w if k == 0 else parts))
    kv = [plan.to_head(x, k) for k, x in enumerate(pairs)]
    w_other = [plan.partner(x) for x in (kv[0], *w_own)]
    w_full, part, own = grads_call(plan, kv, w_own, w_other)

    kept, *shares = share_call(plan, own, plan.partner(part))
    packed_q = pack_queries(plan, view_lengths, queries, moments)
    arrived = [plan.along(x, k + 1) for k, x in enumerate(shares)]
    q = [plan.to_head(x, k) for k, x in enumerate(packed_q)]
    view_out = attend_call(plan, q, kv, gains)

    got, mom = moment_call(plan, kept, arrived, q[0], scale)
    m_own = [mom] + [plan.along(mom, k) for k in range(1, rest)]
    m_other = [plan.partner(x) for x in m_own]
    got = plan.send(got, plan.place, plan.home)
    new_moments = [
        momentum_decay * moment + got[i][None] for i, moment in enumerate(moments)
    ]
    outs = fast_call(plan, q, view_out, w_full, m_own, m_other, gains)
    outs = [plan.to_tokens(x, k) for k, x in enumerate(outs)]
    output, *fresh = finish_call(plan, outs)
    return (output, *fresh, *new_moments)


def attend(query_rows, key_rows, value_rows, query_ids, key_ids):
    scaling = query_rows.shape[-1] ** (-0.5)
    scores = (
        jnp.einsum("rhd,ghd->hrg", query_rows, key_rows, preferred_element_type=jnp.float32)
        * scaling
    )
    allowed = query_ids[:, None] == key_ids[None, :]
    scores = jnp.where(allowed[None], scores, -1e30)
    highest = jnp.max(scores, axis=-1, keepdims=True)
    expo = jnp.exp(scores - highest)
    probs = (expo / jnp.sum(expo, axis=-1, keepdims=True)).astype(jnp.bfloat16)
    return jnp.einsum("hrg,ghd->rhd", probs, value_rows, preferred_element_type=jnp.float32)


def rms_gain(field, gains):
    return field * lax.rsqrt(jnp.mean(field * field, axis=-1, keepdims=True) + epsilon) * gains


def silu_slope(pre):
    sig = jax.nn.sigmoid(pre)
    return sig * (1.0 + pre * (1.0 - sig))


def block_gradients(key_rows, value_rows, gate_full, up_full, down_full):
    pre_gate = jnp.dot(key_rows, gate_full, preferred_element_type=jnp.float32)
    pre_up = jnp.dot(key_rows, up_full, preferred_element_type=jnp.float32)
    activ = jax.nn.silu(pre_gate)
    hidden = (activ * pre_up).astype(jnp.bfloat16)
    d_hidden = -lax.dot_general(
        value_rows, down_full, (((1,), (1,)), ((), ())), preferred_element_type=jnp.float32
    )
    d_gate = (d_hidden * pre_up * silu_slope(pre_gate)).astype(jnp.bfloat16)
    d_up = (d_hidden * activ).astype(jnp.bfloat16)
    contract = (((0,), (0,)), ((), ()))
    grad_gate = lax.dot_general(key_rows, d_gate, contract, preferred_element_type=jnp.float32)
    grad_up = lax.dot_general(key_rows, d_up, contract, preferred_element_type=jnp.float32)
    grad_down = -lax.dot_general(hidden, value_rows, contract, preferred_element_type=jnp.float32)
    return (grad_gate, grad_up, grad_down)


def gradients(key_rows, value_rows, gate_full, up_full, down_full):
    row_total, head_size = key_rows.shape
    block = min(row_total, 512)

    def add_block(number, totals):
        terms = block_gradients(key_rows, value_rows, gate_full, up_full, down_full)
        return tuple((total + term for total, term in zip(totals, terms)))

    zeros = jnp.zeros((head_size, head_size), jnp.float32)
    return lax.fori_loop(0, row_total // block, add_block, (zeros, zeros, zeros))


def renormed(weight, moment, radius):
    old = weight.astype(jnp.float32)
    moved = old - step_size * moment / radius
    ratio = jnp.sqrt(jnp.sum(old * old, axis=-1, keepdims=True) + epsilon) / jnp.sqrt(
        jnp.sum(moved * moved, axis=-1, keepdims=True) + epsilon
    )
    return (moved * ratio).astype(jnp.bfloat16)


def apply_fast(query_rows, gate_full, up_full, down_full, gains):
    row_total, width = query_rows.shape
    block = min(row_total, 512)

    def one_block(block_rows):
        pre_gate = jnp.dot(block_rows, gate_full, preferred_element_type=jnp.float32)
        pre_up = jnp.dot(block_rows, up_full, preferred_element_type=jnp.float32)
        hidden = (jax.nn.silu(pre_gate) * pre_up).astype(jnp.bfloat16)
        fast_raw = jnp.dot(hidden, down_full, preferred_element_type=jnp.float32)
        return rms_gain(fast_raw, gains).astype(jnp.bfloat16)

    return lax.map(one_block, query_rows.reshape(row_total // block, block, width)).reshape(
        row_total, width
    )


def fast_branch(query_rows, key_rows, value_rows, gains, weights, moments):
    gate_full, up_full, down_full = (
        lax.all_gather(weights[0], "wide", axis=0, tiled=True),
        lax.all_gather(weights[1], "wide", axis=0, tiled=True),
        lax.all_gather(weights[2], "wide", axis=0, tiled=True),
    )
    grads = gradients(key_rows, value_rows, gate_full, up_full, down_full)
    wide_size = lax.axis_size("wide")
    grad_scale = float(key_rows.shape[0] * wide_size) ** (-0.5)
    head_size = key_rows.shape[1]
    row_count = weights[0].shape[0]
    offset = lax.axis_index("wide") * row_count
    blank = jnp.zeros((head_size, head_size), jnp.float32)
    placed = tuple(
        (
            lax.dynamic_update_slice_in_dim(blank, momentum_decay * moment, offset, 0)
            + part * grad_scale
            for moment, part in zip(moments, grads)
        )
    )
    full_moments = lax.psum(placed, "wide")
    full_new = tuple(
        (
            renormed(weight, moment, jnp.sqrt(jnp.mean(moment * moment) + epsilon))
            for weight, moment in zip((gate_full, up_full, down_full), full_moments)
        )
    )
    fresh = tuple((lax.dynamic_slice_in_dim(weight, offset, row_count, 0) for weight in full_new))
    moment_new = tuple(
        (lax.dynamic_slice_in_dim(moment, offset, row_count, 0) for moment in full_moments)
    )
    fast_out = apply_fast(query_rows, full_new[0], full_new[1], full_new[2], gains)
    return (fast_out, fresh, moment_new)


def per_device_general(
    queries, keys, values, view_lengths, gain, w_gate, w_up, w_down, m_gate, m_up, m_down
):
    narrow_size = lax.axis_size("narrow")
    narrow_index = lax.axis_index("narrow")
    tok_dev = queries.shape[0]
    group_size = tok_dev * narrow_size
    head_size = queries.shape[1] // narrow_size
    ends = jnp.cumsum(view_lengths[0])
    position = jnp.arange(group_size, dtype=jnp.int32)
    view_ids = jnp.sum((position[:, None] >= ends[None, :-1]).astype(jnp.int32), axis=1)
    head_gains = lax.dynamic_slice_in_dim(gain, narrow_index * head_size, head_size, 0)
    weights = (w_gate[0], w_up[0], w_down[0])
    moments = (m_gate[0], m_up[0], m_down[0])
    key_group, value_group = (
        lax.all_gather(keys, "narrow", axis=0, tiled=True),
        lax.all_gather(values, "narrow", axis=0, tiled=True),
    )
    own_ids = lax.dynamic_slice_in_dim(view_ids, narrow_index * tok_dev, tok_dev, 0)
    attn = attend(
        queries.reshape(tok_dev, narrow_size, head_size),
        key_group.reshape(group_size, narrow_size, head_size),
        value_group.reshape(group_size, narrow_size, head_size),
        own_ids,
        view_ids,
    )
    view_out = (
        rms_gain(attn, gain.reshape(narrow_size, head_size))
        .astype(jnp.bfloat16)
        .reshape(tok_dev, narrow_size * head_size)
    )
    query_head = lax.all_to_all(queries, "narrow", split_axis=1, concat_axis=0, tiled=True)
    key_head = lax.dynamic_slice_in_dim(key_group, narrow_index * head_size, head_size, 1)
    value_head = lax.dynamic_slice_in_dim(value_group, narrow_index * head_size, head_size, 1)
    fast_out, fresh, moment_new = fast_branch(
        query_head, key_head, value_head, head_gains, weights, moments
    )
    fast_tokens = lax.all_to_all(fast_out, "narrow", split_axis=0, concat_axis=1, tiled=True)
    output = (view_out.astype(jnp.float32) + fast_tokens.astype(jnp.float32)).astype(jnp.bfloat16)
    return (
        output,
        fresh[0][None],
        fresh[1][None],
        fresh[2][None],
        moment_new[0][None],
        moment_new[1][None],
        moment_new[2][None],
    )


def solution(mesh):
    wide, narrow = mesh.shape["wide"], mesh.shape["narrow"]
    paired = wide % 2 == 0 and narrow % 2 == 0 and wide <= 16

    def body(queries, keys, values, view_lengths, *args):
        operands = (queries, keys, values, view_lengths, *args)
        if not paired:
            return per_device_general(*operands)
        tokens, width = queries.shape
        rows, views = args[1].shape[1], view_lengths.shape[1]
        plan = Plan(mesh, rows, tokens, width // narrow, views)
        return per_device(plan, *operands)

    tokens = P(("wide", "narrow"), None)
    state = P("narrow", "wide", None)
    in_specs = (tokens, tokens, tokens, P("wide", None), P()) + (state,) * 6
    out_specs = (tokens,) + (state,) * 6
    return jax.shard_map(
        body, mesh=mesh, in_specs=in_specs, out_specs=out_specs, check_vma=False
    )
```
